32 devices in a mesh: seq: 32 (over z, y, x, core).
Axes of the slice: x: 2, y: 2, z: 4, core: 2. Of those that a mesh axis runs over, the one named last changes fastest.
Arguments:
- history: float32 [12288, 1024], P('seq'), may hold values from -6 to 6
- taps: float32 [12288, 1024], P('seq'), may hold values from -0.109375 to 0.109375
- self_taps: float32 [1024, 256], P('seq'), may hold values from -0.375 to 0.375
- fresh: float32 [1024, 256], P('seq'), may hold values from -6 to 6
- gate: float32 [1024, 256], P('seq'), may hold values from -6 to 6
Outputs:
- gated: float32 [1024, 256], P('seq')
The draws below stay inside these ranges and needn't reach their ends.
All inputs are finite; a program needn't handle non-finite values.
Results may differ from the reference program's by a relative error of at most 0.000053.
Values sent between devices are 32-bit elements; how exact they have to be, the bound alone decides.
A program may use at most 64 MiB of HBM per device.

```python
import jax
import jax.numpy as jnp
from jax import lax

CHANNELS = 1024
NEW_TOKENS = 256
HISTORY = 12288


def raised(entries, key, source, target, shards_of, factor):
    owner, partner = [(jnp.arange(entries.shape[dim]) // (entries.shape[dim] // shards_of)).reshape([-1 if axis == dim else 1 for axis in range(entries.ndim)]) for dim in (source, target)]
    chosen = jax.random.permutation(key, shards_of)[partner]
    strong = (owner == chosen) | (owner == (partner + shards_of // 2) % shards_of)
    return jnp.where(strong, factor * entries, entries)


def steps_of(own_key, shape, shards, smallest, high):
    gain, own = 1.0, jax.random.fold_in(own_key, 6)
    for dim, shards_of in shards:
        heights = jnp.exp(jax.random.uniform(jax.random.fold_in(own, dim), (shards_of,), jnp.float32, smallest / len(shards), high / len(shards)))
        gain = gain * jnp.repeat(heights, shape[dim] // shards_of).reshape([-1 if axis == dim else 1 for axis in range(len(shape))])
    return gain


def gaussian(rng, shape, deviation, reach, split=(), dtype=jnp.bfloat16):
    level = steps_of(rng, shape, split, -0.22, 0.18) if split else 1.0
    entries = jax.random.normal(rng, shape, jnp.float32) * deviation * level
    return jnp.minimum(jnp.maximum(entries, -reach), reach).astype(dtype)


def heavy_noise(own_key, shape, spread, most, split, heavy, held_as=jnp.bfloat16):
    array = spread * jax.random.normal(own_key, shape, jnp.float32)
    if split:
        array = array * steps_of(own_key, shape, split, -0.22, 0.18)
    return jnp.clip(raised(array, jax.random.fold_in(own_key, 3), *heavy), -most, most).astype(held_as)


def setup_inputs(seed: int = 0) -> dict:
    arg_keys = jax.random.split(jax.random.key(seed), 6)
    return {
        "history": gaussian(arg_keys[0], (HISTORY, CHANNELS), 1.0, 6.0, ((0, 32),), jnp.float32),
        "taps": heavy_noise(arg_keys[1], (HISTORY, CHANNELS), HISTORY ** -0.5, 0.109375, ((0, 32),), (0, 1, 32, 2.75), jnp.float32),
        "self_taps": gaussian(arg_keys[2], (CHANNELS, NEW_TOKENS), NEW_TOKENS ** -0.5, 0.375, ((0, 32),), jnp.float32),
        "fresh": gaussian(arg_keys[3], (CHANNELS, NEW_TOKENS), 1.0, 6.0, ((0, 32),), jnp.float32),
        "gate": gaussian(arg_keys[4], (CHANNELS, NEW_TOKENS), 1.0, 6.0, ((0, 32),), jnp.float32),
    }


def correlate(pair):
    hist_block, taps_block = pair
    length = 2 * HISTORY
    hist_spec = jnp.fft.rfft(hist_block, n=length, axis=0)
    taps_spec = jnp.fft.rfft(taps_block, n=length, axis=0)
    return jnp.fft.irfft(jnp.conj(taps_spec) * hist_spec, n=length, axis=0)[:NEW_TOKENS]


def reference(history, taps, self_taps, fresh, gate):
    groups = CHANNELS // 32
    hist_blocks = history.reshape(HISTORY, groups, 32).transpose(1, 0, 2)
    taps_blocks = taps.reshape(HISTORY, groups, 32).transpose(1, 0, 2)
    lagged = lax.map(correlate, (hist_blocks, taps_blocks))
    hist_part = lagged.transpose(0, 2, 1).reshape(CHANNELS, NEW_TOKENS)
    doubled = 2 * NEW_TOKENS
    own_spec = jnp.fft.rfft(self_taps, n=doubled, axis=1) * jnp.fft.rfft(fresh, n=doubled, axis=1)
    own_part = jnp.fft.irfft(own_spec, n=doubled, axis=1)[:, :NEW_TOKENS]
    return gate * (hist_part + own_part)
```

```python
import math

import jax
import jax.numpy as jnp
import numpy as np
from jax import lax
from jax.experimental import pallas as pl
from jax.experimental.pallas import tpu as pltpu
from jax.sharding import PartitionSpec as P

AXIS = "seq"
PLANE = 8
MESH = pl.DeviceIdType.MESH
F32 = jnp.float32
BF16 = jnp.bfloat16
scope = jax.named_scope
AHEAD = 3


def dft_matrix(seg):
    phase = np.outer(4 * np.arange(seg) + 1, np.arange(seg)) % (4 * seg)
    angle = phase * (math.pi / (2 * seg))
    return np.concatenate([np.cos(angle), -np.sin(angle)], axis=0)


def halves(matrix):
    high = np.asarray(matrix, np.float32).astype(BF16)
    low = np.asarray(matrix - high.astype(np.float64), np.float32).astype(BF16)
    return high, low


def split(value):
    high = value.astype(BF16)
    return high, (value - high.astype(F32)).astype(BF16)


def mul_conj(a, b):
    return a[0] * b[0] + a[1] * b[1], a[1] * b[0] - a[0] * b[1]


def mul(a, b):
    return a[0] * b[0] - a[1] * b[1], a[0] * b[1] + a[1] * b[0]


def add(a, b):
    return a[0] + b[0], a[1] + b[1]


def turn(a):
    return -a[1], a[0]


def back(a):
    return a[1], -a[0]


def local_products(hs, ts):
    us = [None] + [add(ts[a], turn(ts[a - 1])) for a in range(1, len(ts))]
    first = mul_conj(hs[0], ts[0])
    for a in range(1, len(hs)):
        first = add(first, mul_conj(hs[a], us[a]))
    second = mul_conj(hs[1], ts[0])
    for a in range(2, len(hs)):
        second = add(second, mul_conj(hs[a], us[a - 1]))
    return first, second


def halo_products(first, second, h0, h1, t_near, t_before, h_after):
    one = mul_conj(h0, t_before)
    two = add(mul_conj(h1, t_before), mul_conj(h_after, t_near))
    return add(first, back(one)), add(add(second, one), back(two))


def own_products(f0, f1, s0, s1):
    first = mul(f0, s0)
    return first, add(turn(first), add(mul(f0, s1), mul(f1, s0)))


def plain_body(history, taps, self_taps, fresh, gate):
    n = lax.axis_size(AXIS)
    seg = fresh.shape[1] // 2
    matrix = jnp.asarray(dft_matrix(seg).astype(np.float32))
    hp = lax.Precision.HIGHEST
    before = lax.ppermute(taps[-seg:], AXIS, [(s, s + 1) for s in range(n - 1)])
    after = lax.ppermute(history[:seg], AXIS, [(s, s - 1) for s in range(1, n)])

    def forward(rows):
        spec = jnp.dot(matrix, rows, precision=hp)
        return spec[:seg], spec[seg:]

    def inverse(spec):
        return jnp.dot(matrix.T / seg, jnp.concatenate(spec, axis=0), precision=hp)

    count = history.shape[0] // seg
    hs = [forward(history[a * seg : (a + 1) * seg]) for a in range(count)]
    ts = [forward(taps[a * seg : (a + 1) * seg]) for a in range(count)]
    first, second = local_products(hs, ts)
    first, second = halo_products(first, second, hs[0], hs[1], ts[-2], forward(before), forward(after))
    part = jnp.concatenate([inverse(first), inverse(second)], axis=0).T
    summed = lax.psum_scatter(part, AXIS, scatter_dimension=0, tiled=True)
    f, s = fresh.T, self_taps.T
    own = own_products(forward(f[:seg]), forward(f[seg:]), forward(s[:seg]), forward(s[seg:]))
    own_part = jnp.concatenate([inverse(own[0]), inverse(own[1])], axis=0).T
    return gate * (summed + own_part)


def flip(z, mask):
    value, bit = z, 1
    while bit <= mask:
        if mask & bit:
            value = value + bit - 2 * bit * (z // bit % 2)
        bit *= 2
    return value


def kernel(n, seg, hist, taps, self_taps_h, fresh_h, gate_h, fh_h, fl_h, gh_h, gl_h, out,
           self_taps, fresh, gate, fh, fl, gh, gl, hist_v, taps_v, tb, ha, sh0, sh1, st1, q0, q1,
           parts, d_recv, y_send, y_recv, w_send, w_recv, v_send, v_recv, sums, n_recv,
           small_sem, load_sem, tb_s, tb_r, ha_s, ha_r, d_s, d_r, y_s, y_r, w_s, w_r, v_s, v_r, n_s, n_r):
    me = lax.axis_index(AXIS)
    nz = n // PLANE
    my_z, low = me // PLANE, me % PLANE
    core, x, y = me % 2, low // 2 % 2, low // 4
    rows = hist.shape[0]
    count = rows // seg
    width = hist.shape[1] // nz
    half = width // 2
    block = width // PLANE
    last = nz - 1
    far = nz - 2
    partner = me + 1 - 2 * core
    x_peer, y_peer = me + 2 - 4 * x, me + 4 - 8 * y
    diagonal = me + 2 - 4 * x + 4 - 8 * y
    near = (y_peer, diagonal, x_peer)
    steps = [(0, 0), (1, 0), (2, 0), (0, 1), (1, 1), (2, 1), (3, 0), (3, 1)]

    def level(i):
        return me + (flip(my_z, last - i) - my_z) * PLANE

    def cols(i, h, dev):
        row = dev % PLANE // 4
        base = flip(dev // PLANE, last - i) * width + ((row + 1 + h) % 2) * half
        return pl.ds(pl.multiple_of(base, half), half)

    def lanes(h):
        return pl.ds(h * half, half)

    def remote(src, dst, send, recv, dev):
        return pltpu.make_async_remote_copy(
            src_ref=src, dst_ref=dst, send_sem=send, recv_sem=recv, device_id=(dev,), device_id_type=MESH
        )

    has_next, has_prev = me < n - 1, me > 0
    outer = me + 2 * core - 1
    has_outer = (outer >= 0) & (outer < n)
    peers = [partner]
    peers += near
    peers += [level(i) + j * (2 - 4 * x) for i in range(last) for j in range(2)]
    barrier = pltpu.get_barrier_semaphore()
    @pl.when(has_outer)
    def _():
        pl.semaphore_signal(barrier, inc=1, device_id=(outer,), device_id_type=MESH)

    for peer in peers:
        pl.semaphore_signal(barrier, inc=1, device_id=(peer,), device_id_type=MESH)

    small = [
        pltpu.make_async_copy(src, dst, small_sem.at[k])
        for k, (src, dst) in enumerate((
            (fh_h, fh), (fl_h, fl), (gh_h, gh), (gl_h, gl), (self_taps_h, self_taps), (fresh_h, fresh), (gate_h, gate),
        ))
    ]
    for copy in small:
        copy.start()
    loads = [[] for _ in range(nz)]
    for i, h in steps:
        for k, (src, dst) in enumerate(((hist, hist_v), (taps, taps_v))):
            copy = pltpu.make_async_copy(src.at[:, cols(i, h, me)], dst.at[i, :, lanes(h)], load_sem.at[k, 2 * i + h])
            copy.start()
            loads[i].append(copy)

    with scope("barrier"):
        pl.semaphore_wait(barrier, len(peers) + jnp.where(has_outer, 1, 0))

    def taps_copy(i, h, dev):
        k = 2 * i + h
        return remote(
            taps.at[pl.ds(rows - seg, seg), cols(i, h, dev)], tb.at[i, :, lanes(h)], tb_s.at[k], tb_r.at[k], dev
        )

    def hist_copy(i, h, dev):
        k = 2 * i + h
        return remote(hist.at[pl.ds(0, seg), cols(i, h, dev)], ha.at[i, :, lanes(h)], ha_s.at[k], ha_r.at[k], dev)

    up = has_next & (low == PLANE - 1)
    down = has_prev & (low == 0)

    def send_halo(k, forward_when, back_when):
        i, h = steps[k]

        @pl.when(forward_when)
        def _():
            taps_copy(i, h, me + 1).start()

        @pl.when(back_when)
        def _():
            hist_copy(i, h, me - 1).start()

    for k in range(len(steps)):
        if k < AHEAD:
            send_halo(k, has_next, has_prev)
        else:
            send_halo(k, has_next & ~up, has_prev & ~down)

    def forward(value):
        both = jnp.concatenate(split(value), axis=0)
        spec = jnp.dot(fh[...], both, preferred_element_type=F32) + jnp.dot(
            fl[...], both, preferred_element_type=F32
        )
        return spec[:seg], spec[seg:]

    def keep(ref, i, spec):
        ref[i, :seg], ref[i, seg:] = spec

    def held(ref, i, at):
        return ref[i, :seg, at], ref[i, seg:, at]

    @pl.when(me == 0)
    def _():
        tb[...] = jnp.zeros_like(tb)

    @pl.when(me == n - 1)
    def _():
        ha[...] = jnp.zeros_like(ha)

    for copy in small:
        copy.wait()
    for i in range(nz):
        for copy in loads[i]:
            copy.wait()
        with scope(f"local{i}"):
            hs = [forward(hist_v[i, pl.ds(a * seg, seg)]) for a in range(count)]
            ts = [forward(taps_v[i, pl.ds(a * seg, seg)]) for a in range(count)]
            first, second = local_products(hs, ts)
            keep(sh0, i, hs[0])
            keep(sh1, i, hs[1])
            keep(st1, i, ts[-2])
            keep(q0, i, first)
            keep(q1, i, second)

    contract = (((1,), (1,)), ((), ()))

    def dot_t(a, b):
        return lax.dot_general(a, b, contract, preferred_element_type=F32)

    def own_part():
        f, s = fresh[...], self_taps[...]
        both = jnp.concatenate(
            split(jnp.concatenate([f[:, :seg], f[:, seg:], s[:, :seg], s[:, seg:]], axis=0)), axis=1
        )
        spec = dot_t(both, fh[...]) + dot_t(both, fl[...])
        quads = [
            (spec[k * block : (k + 1) * block, :seg], spec[k * block : (k + 1) * block, seg:]) for k in range(4)
        ]
        a, b = own_products(*quads)
        high, low_half = split(
            jnp.concatenate([jnp.concatenate(a, axis=1), jnp.concatenate(b, axis=1)], axis=0)
        )
        res = dot_t(high, gh[...]) + dot_t(low_half, gh[...]) + dot_t(high, gl[...])
        return jnp.concatenate([res[:block], res[block:]], axis=1)

    def inverse(spec):
        hi, lo = split(jnp.concatenate(spec, axis=0))
        return (
            jnp.dot(gh[...], hi, preferred_element_type=F32)
            + jnp.dot(gh[...], lo, preferred_element_type=F32)
            + jnp.dot(gl[...], hi, preferred_element_type=F32)
        ).T

    def chip_copy(i, h):
        k = 2 * i + h
        return remote(parts.at[k, 1 - core], d_recv.at[k], d_s.at[k], d_r.at[k], partner)

    def y_copy(i):
        return remote(y_send.at[i], y_recv.at[i], y_s.at[i], y_r.at[i], y_peer)

    def w_copy(i, j):
        dev = level(i) + j * (2 - 4 * x)
        place = x + j * (1 - 2 * x)
        return remote(w_send.at[i, place], w_recv.at[i, j], w_s.at[i, j], w_r.at[i, j], dev)

    def v_copy():
        return remote(v_send, v_recv, v_s, v_r, level(far))

    def near_copy(j):
        src = sums.at[0, x] if j == 0 else sums.at[j - 1, 1 - x]
        return remote(src, n_recv.at[j], n_s.at[j], n_r.at[j], near[j])

    def compute(i, h):
        with scope(f"halo{i}{h}"):
            @pl.when(has_prev)
            def _():
                taps_copy(i, h, me).wait_recv()

            @pl.when(has_next)
            def _():
                hist_copy(i, h, me).wait_recv()

        at_step = steps.index((i, h))
        if at_step + AHEAD < len(steps):
            send_halo(at_step + AHEAD, up, down)

        with scope(f"comp{i}{h}"):
            at = lanes(h)
            both = halo_products(
                held(q0, i, at), held(q1, i, at), held(sh0, i, at), held(sh1, i, at), held(st1, i, at),
                forward(tb[i, :, at]), forward(ha[i, :, at]),
            )
            for side, spec in enumerate(both):
                res = inverse(spec)
                for k in range(res.shape[0] // block):
                    parts[2 * i + h, k % 2, k // 2, :, pl.ds(side * seg, seg)] = res[k * block : (k + 1) * block]
            chip_copy(i, h).start()

    def chip_sum(i, h):
        with scope(f"chip{i}{h}"):
            chip_copy(i, h).wait_recv()
        return parts[2 * i + h, core] + d_recv[2 * i + h]

    def route_y(i):
        y_send[i] = chip_sum(i, 0)
        y_copy(i).start()

    def route_w(i):
        value = chip_sum(i, 1)
        with scope(f"y{i}"):
            y_copy(i).wait_recv()
        w_send[i] = value + y_recv[i]
        for j in (1, 0):
            w_copy(i, j).start()

    def route_v(h):
        if h == 0:
            v_send[...] = chip_sum(far, 0)
            v_copy().start()
        else:
            w_send[far] = chip_sum(far, 1)
            for j in (1, 0):
                w_copy(far, j).start()

    own = own_part()
    compute(0, 0)
    compute(1, 0)
    route_y(0)
    compute(2, 0)
    route_y(1)
    compute(0, 1)
    route_v(0)
    compute(1, 1)
    route_w(0)
    compute(2, 1)
    route_w(1)
    compute(3, 0)
    route_v(1)
    compute(3, 1)
    first = chip_sum(last, 0)
    with scope("v0"):
        v_copy().wait_recv()
    sums[0] = first + v_recv[...]
    near_copy(0).start()
    near_copy(1).start()
    second = chip_sum(last, 1)
    sums[1] = second
    near_copy(2).start()
    total = sums[1, x] + own
    for j in range(3):
        with scope(f"near{j}"):
            near_copy(j).wait_recv()
        total = total + n_recv[j]
    for i in range(far + 1):
        for j in range(2):
            with scope(f"w{i}{j}"):
                w_copy(i, j).wait_recv()
            total = total + w_recv[i, j]
    out[...] = gate[...] * total

    with scope("sends"):
        for i, h in steps:
            @pl.when(has_next)
            def _(i=i, h=h):
                taps_copy(i, h, me + 1).wait_send()

            @pl.when(has_prev)
            def _(i=i, h=h):
                hist_copy(i, h, me - 1).wait_send()

            chip_copy(i, h).wait_send()
        for i in range(far):
            y_copy(i).wait_send()
        for i in range(far + 1):
            for j in range(2):
                w_copy(i, j).wait_send()
        v_copy().wait_send()
        for j in range(3):
            near_copy(j).wait_send()


def kernel_body(history, taps, self_taps, fresh, gate):
    n = lax.axis_size(AXIS)
    rows, channels = history.shape
    block, new_len = fresh.shape
    seg = new_len // 2
    nz = n // PLANE
    width = channels // nz
    fh, fl = halves(dft_matrix(seg))
    gh, gl = halves(dft_matrix(seg).T / seg)
    fh, fl = np.concatenate([fh, fh], axis=1), np.concatenate([fl, fl], axis=1)
    vmem = pl.BlockSpec(memory_space=pltpu.VMEM)
    hbm = pl.BlockSpec(memory_space=pl.ANY)
    dma = pltpu.SemaphoreType.DMA
    spec = pltpu.VMEM((nz, 2 * seg, width), F32)
    far = nz - 2

    def pairs(*lead):
        return pltpu.VMEM((*lead, 2, block, new_len), F32)

    return pl.pallas_call(
        lambda *refs: kernel(n, seg, *refs),
        out_shape=pltpu.VMEM(fresh.shape, F32),
        in_specs=[hbm] * 9,
        out_specs=vmem,
        scratch_shapes=[
            pltpu.VMEM(fresh.shape, F32), pltpu.VMEM(fresh.shape, F32), pltpu.VMEM(fresh.shape, F32),
            pltpu.VMEM(fh.shape, BF16), pltpu.VMEM(fh.shape, BF16), pltpu.VMEM(gh.shape, BF16), pltpu.VMEM(gh.shape, BF16),
            pltpu.VMEM((nz, rows, width), F32),
            pltpu.VMEM((nz, rows, width), F32),
            pltpu.VMEM((nz, seg, width), F32),
            pltpu.VMEM((nz, seg, width), F32),
            spec, spec, spec, spec, spec,
            pairs(2 * nz, 2), pairs(2 * nz),
            pairs(far), pairs(far), pairs(far + 1), pairs(far + 1),
            pairs(), pairs(),
            pairs(2),
            pltpu.VMEM((3, block, new_len), F32),
            dma((7,)),
            dma((2, 2 * nz)),
            dma((2 * nz,)), dma((2 * nz,)), dma((2 * nz,)), dma((2 * nz,)),
            dma((2 * nz,)), dma((2 * nz,)),
            dma((far,)), dma((far,)), dma((far + 1, 2)), dma((far + 1, 2)),
            dma, dma,
            dma((3,)), dma((3,)),
        ],
        compiler_params=pltpu.CompilerParams(collective_id=0, has_side_effects=True),
        name="hyena",
    )(history, taps, self_taps, fresh, gate, *(jnp.asarray(m) for m in (fh, fl, gh, gl)))


def solution(mesh):
    n = mesh.shape[AXIS]

    def body(history, taps, self_taps, fresh, gate):
        channels = history.shape[1]
        block = fresh.shape[0]
        planes = n // PLANE
        fits = n % PLANE == 0 and planes >= 4 and planes & (planes - 1) == 0 and block % 32 == 0
        chosen = kernel_body if fits and channels == block * n else plain_body
        return chosen(history, taps, self_taps, fresh, gate)

    spec = P(AXIS, None)
    return jax.shard_map(body, mesh=mesh, in_specs=(spec,) * 5, out_specs=spec, check_vma=False)
```

```python
import math

import jax
import jax.numpy as jnp
import numpy as np
from jax import lax
from jax.experimental import pallas as pl
from jax.experimental.pallas import tpu as pltpu
from jax.sharding import PartitionSpec as P

AXIS = "seq"
PLANE = 8
MESH = pl.DeviceIdType.MESH
F32 = jnp.float32
BF16 = jnp.bfloat16
scope = jax.named_scope
AHEAD = 3


def dft_matrix(seg):
    phase = np.outer(4 * np.arange(seg) + 1, np.arange(seg)) % (4 * seg)
    angle = phase * (math.pi / (2 * seg))
    return np.concatenate([np.cos(angle), -np.sin(angle)], axis=0)


def halves(matrix):
    high = np.asarray(matrix, np.float32).astype(BF16)
    low = np.asarray(matrix - high.astype(np.float64), np.float32).astype(BF16)
    return high, low


def split(value):
    high = value.astype(BF16)
    return high, (value - high.astype(F32)).astype(BF16)


def mul_conj(a, b):
    return a[0] * b[0] + a[1] * b[1], a[1] * b[0] - a[0] * b[1]


def mul(a, b):
    return a[0] * b[0] - a[1] * b[1], a[0] * b[1] + a[1] * b[0]


def add(a, b):
    return a[0] + b[0], a[1] + b[1]


def turn(a):
    return -a[1], a[0]


def back(a):
    return a[1], -a[0]


def local_products(hs, ts):
    us = [None] + [add(ts[a], turn(ts[a - 1])) for a in range(1, len(ts))]
    first = mul_conj(hs[0], ts[0])
    for a in range(1, len(hs)):
        first = add(first, mul_conj(hs[a], us[a]))
    second = mul_conj(hs[1], ts[0])
    for a in range(2, len(hs)):
        second = add(second, mul_conj(hs[a], us[a - 1]))
    return first, second


def halo_products(first, second, h0, h1, t_near, t_before, h_after):
    one = mul_conj(h0, t_before)
    two = add(mul_conj(h1, t_before), mul_conj(h_after, t_near))
    return add(first, back(one)), add(add(second, one), back(two))


def own_products(f0, f1, s0, s1):
    first = mul(f0, s0)
    return first, add(turn(first), add(mul(f0, s1), mul(f1, s0)))


def plain_body(history, taps, self_taps, fresh, gate):
    n = lax.axis_size(AXIS)
    seg = fresh.shape[1] // 2
    matrix = jnp.asarray(dft_matrix(seg).astype(np.float32))
    hp = lax.Precision.HIGHEST
    before = lax.ppermute(taps[-seg:], AXIS, [(s, s + 1) for s in range(n - 1)])
    after = lax.ppermute(history[:seg], AXIS, [(s, s - 1) for s in range(1, n)])

    def forward(rows):
        spec = jnp.dot(matrix, rows, precision=hp)
        return spec[:seg], spec[seg:]

    def inverse(spec):
        return jnp.dot(matrix.T / seg, jnp.concatenate(spec, axis=0), precision=hp)

    count = history.shape[0] // seg
    hs = [forward(history[a * seg : (a + 1) * seg]) for a in range(count)]
    ts = [forward(taps[a * seg : (a + 1) * seg]) for a in range(count)]
    first, second = local_products(hs, ts)
    first, second = halo_products(first, second, hs[0], hs[1], ts[-2], forward(before), forward(after))
    part = jnp.concatenate([inverse(first), inverse(second)], axis=0).T
    summed = lax.psum_scatter(part, AXIS, scatter_dimension=0, tiled=True)
    f, s = fresh.T, self_taps.T
    own = own_products(forward(f[:seg]), forward(f[seg:]), forward(s[:seg]), forward(s[seg:]))
    own_part = jnp.concatenate([inverse(own[0]), inverse(own[1])], axis=0).T
    return gate * (summed + own_part)


def flip(z, mask):
    value, bit = z, 1
    while bit <= mask:
        if mask & bit:
            value = value + bit - 2 * bit * (z // bit % 2)
        bit *= 2
    return value


def kernel(n, seg, hist, taps, self_taps_h, fresh_h, gate_h, tables_h, out,
           rows_v, tables, both_v, halo_v, sh0, sh1, st1, q0, q1,
           parts, d_recv, y_send, y_recv, w_send, v_send, v_recv, sums, final,
           ready, small_sem, load_sem, t_s, h_s, halo_r, d_s, d_r, y_s, y_r, w_s, v_s, v_r, n_s, final_r):
    me = lax.axis_index(AXIS)
    nz = n // PLANE
    my_z, low = me // PLANE, me % PLANE
    core, x, y = me % 2, low // 2 % 2, low // 4
    rows = hist.shape[0]
    count = rows // seg
    width = hist.shape[1] // nz
    half = width // 2
    block = width // PLANE
    last = nz - 1
    far = nz - 2
    partner = me + 1 - 2 * core
    x_peer, y_peer = me + 2 - 4 * x, me + 4 - 8 * y
    diagonal = me + 2 - 4 * x + 4 - 8 * y
    near = (y_peer, diagonal, x_peer)
    steps = [(i, h) for h in range(2) for i in range(last)] + [(last, 0), (last, 1)]

    def level(i):
        return me + (flip(my_z, last - i) - my_z) * PLANE

    def cols(i, h, dev):
        row = dev % PLANE // 4
        base = flip(dev // PLANE, last - i) * width + ((row + 1 + h) % 2) * half
        return pl.ds(pl.multiple_of(base, half), half)

    def lanes(h):
        return pl.ds(h * half, half)

    def remote(src, dst, send, recv, dev):
        return pltpu.make_async_remote_copy(
            src_ref=src, dst_ref=dst, send_sem=send, recv_sem=recv, device_id=(dev,), device_id_type=MESH
        )

    has_next, has_prev = me < n - 1, me > 0
    outer = me + 2 * core - 1
    has_outer = (outer >= 0) & (outer < n)
    up = has_next & (low == PLANE - 1)
    down = has_prev & (low == 0)
    beside = [partner, x_peer, x_peer + 1 - 2 * core, y_peer, y_peer + 1 - 2 * core]
    over = [me + PLANE, partner + PLANE]
    under = [me - PLANE, partner - PLANE]
    has_over, has_under = my_z < nz - 1, my_z > 0
    met = len(beside) + jnp.where(has_over, len(over), 0) + jnp.where(has_under, len(under), 0)

    def greet(sem):
        def tell(devices):
            for dev in devices:
                pl.semaphore_signal(sem, inc=1, device_id=(dev,), device_id_type=MESH)

        tell(beside)
        pl.when(has_over)(lambda: tell(over))
        pl.when(has_under)(lambda: tell(under))

    barrier = pltpu.get_barrier_semaphore()

    @pl.when(has_outer)
    def _():
        pl.semaphore_signal(barrier, inc=1, device_id=(outer,), device_id_type=MESH)

    greet(barrier)

    constants = pltpu.make_async_copy(tables_h, tables, small_sem.at[0])
    constants.start()
    for i in range(nz):
        for h in range(2):
            for k, src in enumerate((hist, taps)):
                pltpu.make_async_copy(src.at[:, cols(i, h, me)], both_v.at[i, k, :, lanes(h)], load_sem.at[i]).start()
    for k, src in enumerate((self_taps_h, fresh_h, gate_h)):
        pltpu.make_async_copy(src, rows_v.at[k], small_sem.at[1]).start()

    with scope("barrier"):
        pl.semaphore_wait(barrier, met + jnp.where(has_outer, 1, 0))
    greet(ready.at[0])

    def taps_copy(i, h, dev):
        return remote(
            taps.at[pl.ds(rows - seg, seg), cols(i, h, dev)], halo_v.at[i, 0, :, lanes(h)], t_s, halo_r.at[2 * i + h], dev
        )

    def hist_copy(i, h, dev):
        return remote(
            hist.at[pl.ds(0, seg), cols(i, h, dev)], halo_v.at[i, 1, :, lanes(h)], h_s, halo_r.at[2 * i + h], dev
        )

    def send_halo(k, forward_when, back_when):
        i, h = steps[k]

        @pl.when(forward_when)
        def _():
            taps_copy(i, h, me + 1).start()

        @pl.when(back_when)
        def _():
            hist_copy(i, h, me - 1).start()

    for k in range(len(steps)):
        if k < AHEAD:
            send_halo(k, has_next, has_prev)
        else:
            send_halo(k, has_next & ~up, has_prev & ~down)

    def further(stage):
        with scope(f"ready{stage}"):
            pl.semaphore_wait(ready.at[stage], met)
        if stage + 1 < nz - 1:
            greet(ready.at[stage + 1])

    fh, fl, gh, gl = (slice(k, k + r) for k, r in ((0, 2 * seg), (2 * seg, 2 * seg), (4 * seg, seg), (5 * seg, seg)))

    def forward(value):
        both = jnp.concatenate(split(value), axis=0)
        spec = jnp.dot(tables[fh], both, preferred_element_type=F32) + jnp.dot(
            tables[fl], both, preferred_element_type=F32
        )
        return spec[:seg], spec[seg:]

    def keep(ref, i, spec):
        ref[i, :seg], ref[i, seg:] = spec

    def held(ref, i, at):
        return ref[i, :seg, at], ref[i, seg:, at]

    @pl.when(me == 0)
    def _():
        halo_v[:, 0] = jnp.zeros_like(halo_v[:, 0])

    @pl.when(me == n - 1)
    def _():
        halo_v[:, 1] = jnp.zeros_like(halo_v[:, 1])

    constants.wait()

    def local(i):
        pltpu.make_async_copy(both_v.at[i], both_v.at[i], load_sem.at[i]).wait()
        with scope(f"local{i}"):
            hs = [forward(both_v[i, 0, pl.ds(a * seg, seg)]) for a in range(count)]
            ts = [forward(both_v[i, 1, pl.ds(a * seg, seg)]) for a in range(count)]
            first, second = local_products(hs, ts)
            keep(sh0, i, hs[0])
            keep(sh1, i, hs[1])
            keep(st1, i, ts[-2])
            keep(q0, i, first)
            keep(q1, i, second)

    contract = (((1,), (1,)), ((), ()))

    def dot_t(a, b):
        return lax.dot_general(a, b, contract, preferred_element_type=F32)

    def own_part():
        pltpu.make_async_copy(rows_v, rows_v, small_sem.at[1]).wait()
        s, f = rows_v[0], rows_v[1]
        both = jnp.concatenate(
            split(jnp.concatenate([f[:, :seg], f[:, seg:], s[:, :seg], s[:, seg:]], axis=0)), axis=1
        )
        spec = dot_t(both, tables[fh]) + dot_t(both, tables[fl])
        quads = [
            (spec[k * block : (k + 1) * block, :seg], spec[k * block : (k + 1) * block, seg:]) for k in range(4)
        ]
        a, b = own_products(*quads)
        high, low_half = split(
            jnp.concatenate([jnp.concatenate(a, axis=1), jnp.concatenate(b, axis=1)], axis=0)
        )
        res = dot_t(high, tables[gh]) + dot_t(low_half, tables[gh]) + dot_t(high, tables[gl])
        return jnp.concatenate([res[:block], res[block:]], axis=1)

    def inverse(spec):
        hi, lo = split(jnp.concatenate(spec, axis=0))
        return (
            jnp.dot(tables[gh], hi, preferred_element_type=F32)
            + jnp.dot(tables[gh], lo, preferred_element_type=F32)
            + jnp.dot(tables[gl], hi, preferred_element_type=F32)
        ).T

    def chip_copy(i, h):
        k = 2 * i + h
        return remote(parts.at[k, 1 - core], d_recv.at[k], d_s, d_r.at[k], partner)

    def y_copy(i):
        return remote(y_send.at[i], y_recv.at[i], y_s, y_r.at[i], y_peer)

    def w_copy(i, j):
        dev = level(i) + j * (2 - 4 * x)
        place = x + j * (1 - 2 * x)
        return remote(w_send.at[i, place], final.at[3 + 2 * i + j], w_s, final_r, dev)

    def v_copy():
        return remote(v_send, v_recv, v_s, v_r, level(far))

    def near_copy(j):
        src = sums.at[0, x] if j == 0 else sums.at[j - 1, 1 - x]
        return remote(src, final.at[j], n_s, final_r, near[j])

    def compute(i, h):
        with scope(f"halo{i}{h}"):
            @pl.when(has_prev & has_next)
            def _():
                both = halo_v.at[i, :, :, lanes(h)]
                remote(both, both, t_s, halo_r.at[2 * i + h], me).wait_recv()

            @pl.when(~has_next)
            def _():
                taps_copy(i, h, me).wait_recv()

            @pl.when(~has_prev)
            def _():
                hist_copy(i, h, me).wait_recv()

        at_step = steps.index((i, h))
        if at_step + AHEAD < len(steps):
            send_halo(at_step + AHEAD, up, down)

        with scope(f"comp{i}{h}"):
            at = lanes(h)
            both = halo_products(
                held(q0, i, at), held(q1, i, at), held(sh0, i, at), held(sh1, i, at), held(st1, i, at),
                forward(halo_v[i, 0, :, at]), forward(halo_v[i, 1, :, at]),
            )
            for side, spec in enumerate(both):
                res = inverse(spec)
                for k in range(res.shape[0] // block):
                    parts[2 * i + h, k % 2, k // 2, :, pl.ds(side * seg, seg)] = res[k * block : (k + 1) * block]
            chip_copy(i, h).start()

    def chip_sum(i, h):
        with scope(f"chip{i}{h}"):
            chip_copy(i, h).wait_recv()
        return parts[2 * i + h, core] + d_recv[2 * i + h]

    def route_y(i):
        y_send[i] = chip_sum(i, 0)
        y_copy(i).start()

    def route_w(i):
        value = chip_sum(i, 1)
        if i < far:
            with scope(f"y{i}"):
                y_copy(i).wait_recv()
            value = value + y_recv[i]
        w_send[i] = value
        for j in (1, 0):
            w_copy(i, j).start()

    def route_v():
        v_send[...] = chip_sum(far, 0)
        v_copy().start()

    def spread():
        value = chip_sum(last, 0)
        with scope("v"):
            v_copy().wait_recv()
        sums[0] = value + v_recv[...]
        near_copy(0).start()
        near_copy(1).start()

    def finish():
        sums[1] = chip_sum(last, 1)
        near_copy(2).start()

    for i in range(nz):
        local(i)
        if i % 2:
            further(i // 2)
    own = own_part()
    compute(0, 0)
    compute(1, 0)
    for stage in range(nz // 2, nz - 1):
        further(stage)
    route_y(0)
    for i in range(2, last):
        compute(i, 0)
        route_y(i - 1)
    compute(0, 1)
    route_v()
    for i in range(1, last):
        compute(i, 1)
        if i < far:
            route_w(i - 1)
    compute(last, 0)
    route_w(far)
    compute(last, 1)
    route_w(far - 1)
    spread()
    finish()
    total = sums[1, x] + own
    with scope("final"):
        remote(final, final, n_s, final_r, me).wait_recv()
    for k in range(final.shape[0]):
        total = total + final[k]
    out[...] = rows_v[2] * total

    with scope("sends"):
        @pl.when(has_next)
        def _():
            remote(halo_v.at[:, 0], halo_v.at[:, 0], t_s, final_r, me).wait_send()

        @pl.when(has_prev)
        def _():
            remote(halo_v.at[:, 1], halo_v.at[:, 1], h_s, final_r, me).wait_send()

        three = final.at[pl.ds(0, 3)]
        for src, sem in ((d_recv, d_s), (y_send, y_s), (w_send, w_s), (v_send, v_s), (three, n_s)):
            remote(src, src, sem, final_r, me).wait_send()


def kernel_body(history, taps, self_taps, fresh, gate):
    n = lax.axis_size(AXIS)
    rows, channels = history.shape
    block, new_len = fresh.shape
    seg = new_len // 2
    nz = n // PLANE
    width = channels // nz
    fh, fl = halves(dft_matrix(seg))
    gh, gl = halves(dft_matrix(seg).T / seg)
    tables = np.concatenate([np.concatenate([fh, fh], axis=1), np.concatenate([fl, fl], axis=1), gh, gl], axis=0)
    vmem = pl.BlockSpec(memory_space=pltpu.VMEM)
    hbm = pl.BlockSpec(memory_space=pl.ANY)
    dma = pltpu.SemaphoreType.DMA
    spec = pltpu.VMEM((nz, 2 * seg, width), F32)
    far = nz - 2

    def pairs(*lead):
        return pltpu.VMEM((*lead, 2, block, new_len), F32)

    return pl.pallas_call(
        lambda *refs: kernel(n, seg, *refs),
        out_shape=pltpu.VMEM(fresh.shape, F32),
        in_specs=[hbm] * 6,
        out_specs=vmem,
        scratch_shapes=[
            pltpu.VMEM((3, block, new_len), F32),
            pltpu.VMEM(tables.shape, BF16),
            pltpu.VMEM((nz, 2, rows, width), F32),
            pltpu.VMEM((nz, 2, seg, width), F32),
            spec, spec, spec, spec, spec,
            pairs(2 * nz, 2), pairs(2 * nz),
            pairs(far), pairs(far), pairs(far + 1),
            pairs(), pairs(),
            pairs(2),
            pltpu.VMEM((3 + 2 * (far + 1), block, new_len), F32),
            pltpu.SemaphoreType.REGULAR((nz - 1,)),
            dma((2,)), dma((nz,)),
            dma, dma, dma((2 * nz,)),
            dma, dma((2 * nz,)),
            dma, dma((far,)),
            dma,
            dma, dma,
            dma, dma,
        ],
        compiler_params=pltpu.CompilerParams(collective_id=0, has_side_effects=True),
        name="hyena",
    )(history, taps, self_taps, fresh, gate, jnp.asarray(tables))


def solution(mesh):
    n = mesh.shape[AXIS]

    def body(history, taps, self_taps, fresh, gate):
        channels = history.shape[1]
        block = fresh.shape[0]
        planes = n // PLANE
        fits = n % PLANE == 0 and planes >= 4 and planes & (planes - 1) == 0 and block % 32 == 0
        chosen = kernel_body if fits and channels == block * n else plain_body
        return chosen(history, taps, self_taps, fresh, gate)

    spec = P(AXIS, None)
    return jax.shard_map(body, mesh=mesh, in_specs=(spec,) * 5, out_specs=spec, check_vma=False)
```

```python
import math

import jax
import jax.numpy as jnp
import numpy as np
from jax import lax
from jax.experimental import pallas as pl
from jax.experimental.pallas import tpu as pltpu
from jax.sharding import PartitionSpec as P

AXIS = "seq"
PLANE = 8
MESH = pl.DeviceIdType.MESH
F32 = jnp.float32
BF16 = jnp.bfloat16
scope = jax.named_scope
AHEAD = 3


def dft_matrix(seg):
    phase = np.outer(4 * np.arange(seg) + 1, np.arange(seg)) % (4 * seg)
    angle = phase * (math.pi / (2 * seg))
    return np.concatenate([np.cos(angle), -np.sin(angle)], axis=0)


def halves(matrix):
    high = np.asarray(matrix, np.float32).astype(BF16)
    low = np.asarray(matrix - high.astype(np.float64), np.float32).astype(BF16)
    return high, low


def split(value):
    high = value.astype(BF16)
    return high, (value - high.astype(F32)).astype(BF16)


def mul_conj(a, b):
    return a[0] * b[0] + a[1] * b[1], a[1] * b[0] - a[0] * b[1]


def mul(a, b):
    return a[0] * b[0] - a[1] * b[1], a[0] * b[1] + a[1] * b[0]


def add(a, b):
    return a[0] + b[0], a[1] + b[1]


def turn(a):
    return -a[1], a[0]


def back(a):
    return a[1], -a[0]


def local_products(hs, ts):
    us = [None] + [add(ts[a], turn(ts[a - 1])) for a in range(1, len(ts))]
    first = mul_conj(hs[0], ts[0])
    for a in range(1, len(hs)):
        first = add(first, mul_conj(hs[a], us[a]))
    second = mul_conj(hs[1], ts[0])
    for a in range(2, len(hs)):
        second = add(second, mul_conj(hs[a], us[a - 1]))
    return first, second


def halo_products(first, second, h0, h1, t_near, t_before, h_after):
    one = mul_conj(h0, t_before)
    two = add(mul_conj(h1, t_before), mul_conj(h_after, t_near))
    return add(first, back(one)), add(add(second, one), back(two))


def own_products(f0, f1, s0, s1):
    first = mul(f0, s0)
    return first, add(turn(first), add(mul(f0, s1), mul(f1, s0)))


def plain_body(history, taps, self_taps, fresh, gate):
    n = lax.axis_size(AXIS)
    seg = fresh.shape[1] // 2
    matrix = jnp.asarray(dft_matrix(seg).astype(np.float32))
    hp = lax.Precision.HIGHEST
    before = lax.ppermute(taps[-seg:], AXIS, [(s, s + 1) for s in range(n - 1)])
    after = lax.ppermute(history[:seg], AXIS, [(s, s - 1) for s in range(1, n)])

    def forward(rows):
        spec = jnp.dot(matrix, rows, precision=hp)
        return spec[:seg], spec[seg:]

    def inverse(spec):
        return jnp.dot(matrix.T / seg, jnp.concatenate(spec, axis=0), precision=hp)

    count = history.shape[0] // seg
    hs = [forward(history[a * seg : (a + 1) * seg]) for a in range(count)]
    ts = [forward(taps[a * seg : (a + 1) * seg]) for a in range(count)]
    first, second = local_products(hs, ts)
    first, second = halo_products(first, second, hs[0], hs[1], ts[-2], forward(before), forward(after))
    part = jnp.concatenate([inverse(first), inverse(second)], axis=0).T
    summed = lax.psum_scatter(part, AXIS, scatter_dimension=0, tiled=True)
    f, s = fresh.T, self_taps.T
    own = own_products(forward(f[:seg]), forward(f[seg:]), forward(s[:seg]), forward(s[seg:]))
    own_part = jnp.concatenate([inverse(own[0]), inverse(own[1])], axis=0).T
    return gate * (summed + own_part)


def flip(z, mask):
    value, bit = z, 1
    while bit <= mask:
        if mask & bit:
            value = value + bit - 2 * bit * (z // bit % 2)
        bit *= 2
    return value


def kernel(n, seg, hist, taps, self_taps_h, fresh_h, gate_h, tables_h, out,
           rows_v, tables, both_v, halo_v, sh0, sh1, st1, q0, q1,
           parts, d_recv, y_send, y_recv, w_send, v_send, v_recv, sums, final,
           ready, small_sem, load_sem, t_s, h_s, halo_r, d_s, d_r, y_s, y_r, w_s, v_s, v_r, n_s, final_r):
    me = lax.axis_index(AXIS)
    nz = n // PLANE
    my_z, low = me // PLANE, me % PLANE
    core, x, y = me % 2, low // 2 % 2, low // 4
    rows = hist.shape[0]
    count = rows // seg
    width = hist.shape[1] // nz
    half = width // 2
    block = width // PLANE
    last = nz - 1
    far = nz - 2
    partner = me + 1 - 2 * core
    x_peer, y_peer = me + 2 - 4 * x, me + 4 - 8 * y
    diagonal = me + 2 - 4 * x + 4 - 8 * y
    near = (y_peer, diagonal, x_peer)
    steps = [(i, h) for h in range(2) for i in range(last)] + [(last, 0), (last, 1)]

    def plane(i, z):
        straight = flip(z, last - i)
        if i >= far:
            return straight
        low_first = flip(z, last - i // 2 * 2) // 2 * 2 + i % 2
        return jnp.where(z >= nz // 2, low_first, straight)

    def level(i):
        return me + (plane(i, my_z) - my_z) * PLANE

    def cols(i, h, dev):
        row = (dev % PLANE // 4 + 1 + h) % 2
        if i == last:
            row = jnp.where(dev < PLANE, h, row)
        base = plane(i, dev // PLANE) * width + row * half
        return pl.ds(pl.multiple_of(base, half), half)

    def differ(a, b):
        value, bit = 0, 1
        while bit < nz:
            value = value + bit * ((a // bit + b // bit) % 2)
            bit *= 2
        return value

    def lanes(h):
        return pl.ds(h * half, half)

    def remote(src, dst, send, recv, dev):
        return pltpu.make_async_remote_copy(
            src_ref=src, dst_ref=dst, send_sem=send, recv_sem=recv, device_id=(dev,), device_id_type=MESH
        )

    has_next, has_prev = me < n - 1, me > 0
    outer = me + 2 * core - 1
    has_outer = (outer >= 0) & (outer < n)
    up = has_next & (low == PLANE - 1)
    down = has_prev & (low == 0)
    beside = [partner, x_peer, x_peer + 1 - 2 * core, y_peer, y_peer + 1 - 2 * core]
    over = [me + PLANE, partner + PLANE]
    under = [me - PLANE, partner - PLANE]
    has_over, has_under = my_z < nz - 1, my_z > 0
    met = len(beside) + jnp.where(has_over, len(over), 0) + jnp.where(has_under, len(under), 0)

    def greet(sem):
        def tell(devices):
            for dev in devices:
                pl.semaphore_signal(sem, inc=1, device_id=(dev,), device_id_type=MESH)

        tell(beside)
        pl.when(has_over)(lambda: tell(over))
        pl.when(has_under)(lambda: tell(under))

    barrier = pltpu.get_barrier_semaphore()

    @pl.when(has_outer)
    def _():
        pl.semaphore_signal(barrier, inc=1, device_id=(outer,), device_id_type=MESH)

    greet(barrier)

    constants = pltpu.make_async_copy(tables_h, tables, small_sem.at[0])
    constants.start()
    for i in range(nz):
        for h in range(2):
            for k, src in enumerate((hist, taps)):
                pltpu.make_async_copy(src.at[:, cols(i, h, me)], both_v.at[i, k, :, lanes(h)], load_sem.at[i]).start()
    for k, src in enumerate((self_taps_h, fresh_h, gate_h)):
        pltpu.make_async_copy(src, rows_v.at[k], small_sem.at[1]).start()

    with scope("barrier"):
        pl.semaphore_wait(barrier, met + jnp.where(has_outer, 1, 0))
    greet(ready.at[0])

    def taps_copy(i, h, dev):
        return remote(
            taps.at[pl.ds(rows - seg, seg), cols(i, h, dev)], halo_v.at[i, 0, :, lanes(h)], t_s, halo_r.at[2 * i + h], dev
        )

    def hist_copy(i, h, dev):
        return remote(
            hist.at[pl.ds(0, seg), cols(i, h, dev)], halo_v.at[i, 1, :, lanes(h)], h_s, halo_r.at[2 * i + h], dev
        )

    def send_halo(k, forward_when, back_when):
        i, h = steps[k]

        @pl.when(forward_when)
        def _():
            taps_copy(i, h, me + 1).start()

        @pl.when(back_when)
        def _():
            hist_copy(i, h, me - 1).start()

    for k in range(len(steps)):
        if k < AHEAD:
            send_halo(k, has_next, has_prev)
        else:
            send_halo(k, has_next & ~up, has_prev & ~down)

    def further(stage):
        with scope(f"ready{stage}"):
            pl.semaphore_wait(ready.at[stage], met)
        if stage + 1 < nz - 1:
            greet(ready.at[stage + 1])

    fh, fl, gh, gl = (slice(k, k + r) for k, r in ((0, 2 * seg), (2 * seg, 2 * seg), (4 * seg, seg), (5 * seg, seg)))

    def forward(value):
        both = jnp.concatenate(split(value), axis=0)
        spec = jnp.dot(tables[fh], both, preferred_element_type=F32) + jnp.dot(
            tables[fl], both, preferred_element_type=F32
        )
        return spec[:seg], spec[seg:]

    def keep(ref, i, spec):
        ref[i, :seg], ref[i, seg:] = spec

    def held(ref, i, at):
        return ref[i, :seg, at], ref[i, seg:, at]

    @pl.when(me == 0)
    def _():
        halo_v[:, 0] = jnp.zeros_like(halo_v[:, 0])

    @pl.when(me == n - 1)
    def _():
        halo_v[:, 1] = jnp.zeros_like(halo_v[:, 1])

    constants.wait()

    def local(i):
        pltpu.make_async_copy(both_v.at[i], both_v.at[i], load_sem.at[i]).wait()
        with scope(f"local{i}"):
            hs = [forward(both_v[i, 0, pl.ds(a * seg, seg)]) for a in range(count)]
            ts = [forward(both_v[i, 1, pl.ds(a * seg, seg)]) for a in range(count)]
            first, second = local_products(hs, ts)
            keep(sh0, i, hs[0])
            keep(sh1, i, hs[1])
            keep(st1, i, ts[-2])
            keep(q0, i, first)
            keep(q1, i, second)

    contract = (((1,), (1,)), ((), ()))

    def dot_t(a, b):
        return lax.dot_general(a, b, contract, preferred_element_type=F32)

    def own_part():
        pltpu.make_async_copy(rows_v, rows_v, small_sem.at[1]).wait()
        s, f = rows_v[0], rows_v[1]
        both = jnp.concatenate(
            split(jnp.concatenate([f[:, :seg], f[:, seg:], s[:, :seg], s[:, seg:]], axis=0)), axis=1
        )
        spec = dot_t(both, tables[fh]) + dot_t(both, tables[fl])
        quads = [
            (spec[k * block : (k + 1) * block, :seg], spec[k * block : (k + 1) * block, seg:]) for k in range(4)
        ]
        a, b = own_products(*quads)
        high, low_half = split(
            jnp.concatenate([jnp.concatenate(a, axis=1), jnp.concatenate(b, axis=1)], axis=0)
        )
        res = dot_t(high, tables[gh]) + dot_t(low_half, tables[gh]) + dot_t(high, tables[gl])
        return jnp.concatenate([res[:block], res[block:]], axis=1)

    def inverse(spec):
        hi, lo = split(jnp.concatenate(spec, axis=0))
        return (
            jnp.dot(tables[gh], hi, preferred_element_type=F32)
            + jnp.dot(tables[gh], lo, preferred_element_type=F32)
            + jnp.dot(tables[gl], hi, preferred_element_type=F32)
        ).T

    def chip_copy(i, h):
        k = 2 * i + h
        return remote(parts.at[k, 1 - core], d_recv.at[k], d_s, d_r.at[k], partner)

    def y_copy(i):
        return remote(y_send.at[i], y_recv.at[i], y_s, y_r.at[i], y_peer)

    def w_copy(i, j):
        dev = level(i) + j * (2 - 4 * x)
        place = x + j * (1 - 2 * x)
        slot = 3 + 2 * (last - differ(my_z, plane(i, my_z))) + j
        return remote(w_send.at[i, place], final.at[slot], w_s, final_r, dev)

    def v_copy():
        return remote(v_send, v_recv, v_s, v_r, level(far))

    def near_copy(j):
        src = sums.at[0, x] if j == 0 else sums.at[j - 1, 1 - x]
        return remote(src, final.at[j], n_s, final_r, near[j])

    def compute(i, h):
        with scope(f"halo{i}{h}"):
            @pl.when(has_prev & has_next)
            def _():
                both = halo_v.at[i, :, :, lanes(h)]
                remote(both, both, t_s, halo_r.at[2 * i + h], me).wait_recv()

            @pl.when(~has_next)
            def _():
                taps_copy(i, h, me).wait_recv()

            @pl.when(~has_prev)
            def _():
                hist_copy(i, h, me).wait_recv()

        at_step = steps.index((i, h))
        if at_step + AHEAD < len(steps):
            send_halo(at_step + AHEAD, up, down)

        with scope(f"comp{i}{h}"):
            at = lanes(h)
            both = halo_products(
                held(q0, i, at), held(q1, i, at), held(sh0, i, at), held(sh1, i, at), held(st1, i, at),
                forward(halo_v[i, 0, :, at]), forward(halo_v[i, 1, :, at]),
            )
            for side, spec in enumerate(both):
                res = inverse(spec)
                for k in range(res.shape[0] // block):
                    parts[2 * i + h, k % 2, k // 2, :, pl.ds(side * seg, seg)] = res[k * block : (k + 1) * block]
            chip_copy(i, h).start()

    def chip_sum(i, h):
        with scope(f"chip{i}{h if isinstance(h, int) else ''}"):
            chip_copy(i, h).wait_recv()
        return parts[2 * i + h, core] + d_recv[2 * i + h]

    def route_y(i):
        y_send[i] = chip_sum(i, 0)
        y_copy(i).start()

    def route_w(i):
        value = chip_sum(i, 1)
        if i < far:
            with scope(f"y{i}"):
                y_copy(i).wait_recv()
            value = value + y_recv[i]
        w_send[i] = value
        for j in (1, 0):
            w_copy(i, j).start()

    def route_v():
        v_send[...] = chip_sum(far, 0)
        v_copy().start()

    swap = me < PLANE // 2

    def spread():
        value = chip_sum(last, jnp.where(swap, 1, 0))
        with scope("v"):
            v_copy().wait_recv()
        sums[0] = value + v_recv[...]
        near_copy(0).start()
        near_copy(1).start()

    def finish():
        sums[1] = chip_sum(last, jnp.where(swap, 0, 1))
        near_copy(2).start()

    for i in range(nz):
        local(i)
        if i % 2:
            further(i // 2)
    own = own_part()
    compute(0, 0)
    compute(1, 0)
    for stage in range(nz // 2, nz - 1):
        further(stage)
    route_y(0)
    for i in range(2, last):
        compute(i, 0)
        route_y(i - 1)
    compute(0, 1)
    route_v()
    for i in range(1, last):
        compute(i, 1)
        if i < far:
            route_w(i - 1)
    compute(last, 0)
    route_w(far)
    compute(last, 1)
    pl.when(swap)(finish)
    route_w(far - 1)
    spread()
    pl.when(~swap)(finish)
    total = sums[1, x] + own
    with scope("final"):
        remote(final, final, n_s, final_r, me).wait_recv()
    for k in range(final.shape[0]):
        total = total + final[k]
    out[...] = rows_v[2] * total

    with scope("sends"):
        @pl.when(has_next)
        def _():
            remote(halo_v.at[:, 0], halo_v.at[:, 0], t_s, final_r, me).wait_send()

        @pl.when(has_prev)
        def _():
            remote(halo_v.at[:, 1], halo_v.at[:, 1], h_s, final_r, me).wait_send()

        three = final.at[pl.ds(0, 3)]
        for src, sem in ((d_recv, d_s), (y_send, y_s), (w_send, w_s), (v_send, v_s), (three, n_s)):
            remote(src, src, sem, final_r, me).wait_send()


def kernel_body(history, taps, self_taps, fresh, gate):
    n = lax.axis_size(AXIS)
    rows, channels = history.shape
    block, new_len = fresh.shape
    seg = new_len // 2
    nz = n // PLANE
    width = channels // nz
    fh, fl = halves(dft_matrix(seg))
    gh, gl = halves(dft_matrix(seg).T / seg)
    tables = np.concatenate([np.concatenate([fh, fh], axis=1), np.concatenate([fl, fl], axis=1), gh, gl], axis=0)
    vmem = pl.BlockSpec(memory_space=pltpu.VMEM)
    hbm = pl.BlockSpec(memory_space=pl.ANY)
    dma = pltpu.SemaphoreType.DMA
    spec = pltpu.VMEM((nz, 2 * seg, width), F32)
    far = nz - 2

    def pairs(*lead):
        return pltpu.VMEM((*lead, 2, block, new_len), F32)

    return pl.pallas_call(
        lambda *refs: kernel(n, seg, *refs),
        out_shape=pltpu.VMEM(fresh.shape, F32),
        in_specs=[hbm] * 6,
        out_specs=vmem,
        scratch_shapes=[
            pltpu.VMEM((3, block, new_len), F32),
            pltpu.VMEM(tables.shape, BF16),
            pltpu.VMEM((nz, 2, rows, width), F32),
            pltpu.VMEM((nz, 2, seg, width), F32),
            spec, spec, spec, spec, spec,
            pairs(2 * nz, 2), pairs(2 * nz),
            pairs(far), pairs(far), pairs(far + 1),
            pairs(), pairs(),
            pairs(2),
            pltpu.VMEM((3 + 2 * (far + 1), block, new_len), F32),
            pltpu.SemaphoreType.REGULAR((nz - 1,)),
            dma((2,)), dma((nz,)),
            dma, dma, dma((2 * nz,)),
            dma, dma((2 * nz,)),
            dma, dma((far,)),
            dma,
            dma, dma,
            dma, dma,
        ],
        compiler_params=pltpu.CompilerParams(collective_id=0, has_side_effects=True),
        name="hyena",
    )(history, taps, self_taps, fresh, gate, jnp.asarray(tables))


def solution(mesh):
    n = mesh.shape[AXIS]

    def body(history, taps, self_taps, fresh, gate):
        channels = history.shape[1]
        block = fresh.shape[0]
        planes = n // PLANE
        fits = n % PLANE == 0 and planes >= 4 and planes & (planes - 1) == 0 and block % 32 == 0
        chosen = kernel_body if fits and channels == block * n else plain_body
        return chosen(history, taps, self_taps, fresh, gate)

    spec = P(AXIS, None)
    return jax.shard_map(body, mesh=mesh, in_specs=(spec,) * 5, out_specs=spec, check_vma=False)
```

```python
import math

import jax
import jax.numpy as jnp
import numpy as np
from jax import lax
from jax.experimental import pallas as pl
from jax.experimental.pallas import tpu as pltpu
from jax.sharding import PartitionSpec as P

AXIS = "seq"
PLANE = 8
MESH = pl.DeviceIdType.MESH
F32 = jnp.float32
BF16 = jnp.bfloat16
scope = jax.named_scope
AHEAD = 3


def dft_matrix(seg):
    phase = np.outer(4 * np.arange(seg) + 1, np.arange(seg)) % (4 * seg)
    angle = phase * (math.pi / (2 * seg))
    return np.concatenate([np.cos(angle), -np.sin(angle)], axis=0)


def halves(matrix):
    high = np.asarray(matrix, np.float32).astype(BF16)
    low = np.asarray(matrix - high.astype(np.float64), np.float32).astype(BF16)
    return high, low


def split(value):
    high = value.astype(BF16)
    return high, (value - high.astype(F32)).astype(BF16)


def mul_conj(a, b):
    return a[0] * b[0] + a[1] * b[1], a[1] * b[0] - a[0] * b[1]


def mul(a, b):
    return a[0] * b[0] - a[1] * b[1], a[0] * b[1] + a[1] * b[0]


def add(a, b):
    return a[0] + b[0], a[1] + b[1]


def turn(a):
    return -a[1], a[0]


def back(a):
    return a[1], -a[0]


def local_products(hs, ts):
    us = [None] + [add(ts[a], turn(ts[a - 1])) for a in range(1, len(ts))]
    first = mul_conj(hs[0], ts[0])
    for a in range(1, len(hs)):
        first = add(first, mul_conj(hs[a], us[a]))
    second = mul_conj(hs[1], ts[0])
    for a in range(2, len(hs)):
        second = add(second, mul_conj(hs[a], us[a - 1]))
    return first, second


def halo_products(first, second, h0, h1, t_near, t_before, h_after):
    one = mul_conj(h0, t_before)
    two = add(mul_conj(h1, t_before), mul_conj(h_after, t_near))
    return add(first, back(one)), add(add(second, one), back(two))


def own_products(f0, f1, s0, s1):
    first = mul(f0, s0)
    return first, add(turn(first), add(mul(f0, s1), mul(f1, s0)))


def plain_body(history, taps, self_taps, fresh, gate):
    n = lax.axis_size(AXIS)
    seg = fresh.shape[1] // 2
    matrix = jnp.asarray(dft_matrix(seg).astype(np.float32))
    hp = lax.Precision.HIGHEST
    before = lax.ppermute(taps[-seg:], AXIS, [(s, s + 1) for s in range(n - 1)])
    after = lax.ppermute(history[:seg], AXIS, [(s, s - 1) for s in range(1, n)])

    def forward(rows):
        spec = jnp.dot(matrix, rows, precision=hp)
        return spec[:seg], spec[seg:]

    def inverse(spec):
        return jnp.dot(matrix.T / seg, jnp.concatenate(spec, axis=0), precision=hp)

    count = history.shape[0] // seg
    hs = [forward(history[a * seg : (a + 1) * seg]) for a in range(count)]
    ts = [forward(taps[a * seg : (a + 1) * seg]) for a in range(count)]
    first, second = local_products(hs, ts)
    first, second = halo_products(first, second, hs[0], hs[1], ts[-2], forward(before), forward(after))
    part = jnp.concatenate([inverse(first), inverse(second)], axis=0).T
    summed = lax.psum_scatter(part, AXIS, scatter_dimension=0, tiled=True)
    f, s = fresh.T, self_taps.T
    own = own_products(forward(f[:seg]), forward(f[seg:]), forward(s[:seg]), forward(s[seg:]))
    own_part = jnp.concatenate([inverse(own[0]), inverse(own[1])], axis=0).T
    return gate * (summed + own_part)


def flip(z, mask):
    value, bit = z, 1
    while bit <= mask:
        if mask & bit:
            value = value + bit - 2 * bit * (z // bit % 2)
        bit *= 2
    return value


def kernel(n, seg, hist, taps, self_taps_h, fresh_h, gate_h, tables_h, out,
           rows_v, tables, both_v, halo_v, sh0, sh1, st1, q0, q1,
           parts, d_recv, y_send, y_recv, w_send, v_send, v_recv, sums, final,
           ready, small_sem, load_sem, edge_sem, t_s, h_s, halo_r, d_s, d_r, y_s, y_r, w_s, v_s, v_r, n_s, final_r):
    me = lax.axis_index(AXIS)
    nz = n // PLANE
    my_z, low = me // PLANE, me % PLANE
    core, x, y = me % 2, low // 2 % 2, low // 4
    rows = hist.shape[0]
    count = rows // seg
    width = hist.shape[1] // nz
    half = width // 2
    block = width // PLANE
    last = nz - 1
    far = nz - 2
    partner = me + 1 - 2 * core
    x_peer, y_peer = me + 2 - 4 * x, me + 4 - 8 * y
    diagonal = me + 2 - 4 * x + 4 - 8 * y
    near = (y_peer, diagonal, x_peer)
    steps = [(i, h) for h in range(2) for i in range(last)] + [(last, 0), (last, 1)]

    def plane(i, z):
        straight = flip(z, last - i)
        if i >= far:
            return straight
        low_first = flip(z, last - i // 2 * 2) // 2 * 2 + i % 2
        return jnp.where(z >= nz // 2, low_first, straight)

    def level(i):
        return me + (plane(i, my_z) - my_z) * PLANE

    def half_row(i, h, dev):
        row = (dev % PLANE // 4 + 1 + h) % 2
        return jnp.where(dev < PLANE, h, row) if i == last else row

    def cols(i, h, dev):
        base = plane(i, dev // PLANE) * width + half_row(i, h, dev) * half
        return pl.ds(pl.multiple_of(base, half), half)

    def differ(a, b):
        value, bit = 0, 1
        while bit < nz:
            value = value + bit * ((a // bit + b // bit) % 2)
            bit *= 2
        return value

    def lanes(h):
        return pl.ds(h * half, half)

    def remote(src, dst, send, recv, dev):
        return pltpu.make_async_remote_copy(
            src_ref=src, dst_ref=dst, send_sem=send, recv_sem=recv, device_id=(dev,), device_id_type=MESH
        )

    has_next, has_prev = me < n - 1, me > 0
    outer = me + 2 * core - 1
    has_outer = (outer >= 0) & (outer < n)
    up = has_next & (low == PLANE - 1)
    down = has_prev & (low == 0)
    beside = [partner, x_peer, x_peer + 1 - 2 * core, y_peer, y_peer + 1 - 2 * core]
    over = [me + PLANE, partner + PLANE]
    under = [me - PLANE, partner - PLANE]
    has_over, has_under = my_z < nz - 1, my_z > 0
    met = len(beside) + jnp.where(has_over, len(over), 0) + jnp.where(has_under, len(under), 0)

    def greet(sem):
        def tell(devices):
            for dev in devices:
                pl.semaphore_signal(sem, inc=1, device_id=(dev,), device_id_type=MESH)

        tell(beside)
        pl.when(has_over)(lambda: tell(over))
        pl.when(has_under)(lambda: tell(under))

    barrier = pltpu.get_barrier_semaphore()

    @pl.when(has_outer)
    def _():
        pl.semaphore_signal(barrier, inc=1, device_id=(outer,), device_id_type=MESH)

    greet(barrier)

    constants = pltpu.make_async_copy(tables_h, tables, small_sem.at[0])
    constants.start()

    def load(i, h, k, start, length, sem):
        span = pl.ds(start, length)
        pltpu.make_async_copy((hist, taps)[k].at[span, cols(i, h, me)], both_v.at[i, k, span, lanes(h)], sem).start()

    rest = rows - seg
    for i in range(nz):
        for h in range(2):
            load(i, h, 0, 0, seg, edge_sem)
            load(i, h, 1, rest, seg, edge_sem)
    for i in range(nz):
        for h in range(2):
            load(i, h, 0, seg, rest, load_sem.at[i])
            load(i, h, 1, 0, rest, load_sem.at[i])
    for k, src in enumerate((self_taps_h, fresh_h, gate_h)):
        pltpu.make_async_copy(src, rows_v.at[k], small_sem.at[1]).start()

    with scope("barrier"):
        pl.semaphore_wait(barrier, met + jnp.where(has_outer, 1, 0))
    greet(ready.at[0])
    pltpu.make_async_copy(halo_v, halo_v, edge_sem).wait()

    def mine(i, dev):
        goal = plane(i, dev // PLANE)
        mask = differ(my_z, goal)
        straight = last - mask
        return jnp.where((my_z >= nz // 2) & (mask >= 2), straight // 2 * 2 + goal % 2, straight)

    def spot(i, h, dev):
        row = half_row(i, h, dev)
        place = jnp.where((me < PLANE) & (plane(i, dev // PLANE) == my_z), row, (row + y + 1) % 2)
        return pl.ds(pl.multiple_of(place * half, half), half)

    def taps_copy(i, h, dev):
        src = both_v.at[mine(i, dev), 1, pl.ds(rows - seg, seg), spot(i, h, dev)]
        return remote(src, halo_v.at[i, 0, :, lanes(h)], t_s, halo_r.at[2 * i + h], dev)

    def hist_copy(i, h, dev):
        src = both_v.at[mine(i, dev), 0, pl.ds(0, seg), spot(i, h, dev)]
        return remote(src, halo_v.at[i, 1, :, lanes(h)], h_s, halo_r.at[2 * i + h], dev)

    def send_halo(k, forward_when, back_when):
        i, h = steps[k]

        @pl.when(forward_when)
        def _():
            taps_copy(i, h, me + 1).start()

        @pl.when(back_when)
        def _():
            hist_copy(i, h, me - 1).start()

    for k in range(len(steps)):
        if k < AHEAD:
            send_halo(k, has_next, has_prev)
        else:
            send_halo(k, has_next & ~up, has_prev & ~down)

    def further(stage):
        with scope(f"ready{stage}"):
            pl.semaphore_wait(ready.at[stage], met)
        if stage + 1 < nz - 1:
            greet(ready.at[stage + 1])

    fh, fl, gh, gl = (slice(k, k + r) for k, r in ((0, 2 * seg), (2 * seg, 2 * seg), (4 * seg, seg), (5 * seg, seg)))

    def forward(value):
        both = jnp.concatenate(split(value), axis=0)
        spec = jnp.dot(tables[fh], both, preferred_element_type=F32) + jnp.dot(
            tables[fl], both, preferred_element_type=F32
        )
        return spec[:seg], spec[seg:]

    def keep(ref, i, spec):
        ref[i, :seg], ref[i, seg:] = spec

    def held(ref, i, at):
        return ref[i, :seg, at], ref[i, seg:, at]

    @pl.when(me == 0)
    def _():
        halo_v[:, 0] = jnp.zeros_like(halo_v[:, 0])

    @pl.when(me == n - 1)
    def _():
        halo_v[:, 1] = jnp.zeros_like(halo_v[:, 1])

    constants.wait()

    def local(i):
        some = both_v.at[i, :, pl.ds(0, rest)]
        pltpu.make_async_copy(some, some, load_sem.at[i]).wait()
        with scope(f"local{i}"):
            hs = [forward(both_v[i, 0, pl.ds(a * seg, seg)]) for a in range(count)]
            ts = [forward(both_v[i, 1, pl.ds(a * seg, seg)]) for a in range(count)]
            first, second = local_products(hs, ts)
            keep(sh0, i, hs[0])
            keep(sh1, i, hs[1])
            keep(st1, i, ts[-2])
            keep(q0, i, first)
            keep(q1, i, second)

    contract = (((1,), (1,)), ((), ()))

    def dot_t(a, b):
        return lax.dot_general(a, b, contract, preferred_element_type=F32)

    def own_part():
        pltpu.make_async_copy(rows_v, rows_v, small_sem.at[1]).wait()
        s, f = rows_v[0], rows_v[1]
        both = jnp.concatenate(
            split(jnp.concatenate([f[:, :seg], f[:, seg:], s[:, :seg], s[:, seg:]], axis=0)), axis=1
        )
        spec = dot_t(both, tables[fh]) + dot_t(both, tables[fl])
        quads = [
            (spec[k * block : (k + 1) * block, :seg], spec[k * block : (k + 1) * block, seg:]) for k in range(4)
        ]
        a, b = own_products(*quads)
        high, low_half = split(
            jnp.concatenate([jnp.concatenate(a, axis=1), jnp.concatenate(b, axis=1)], axis=0)
        )
        res = dot_t(high, tables[gh]) + dot_t(low_half, tables[gh]) + dot_t(high, tables[gl])
        return jnp.concatenate([res[:block], res[block:]], axis=1)

    def inverse(spec):
        hi, lo = split(jnp.concatenate(spec, axis=0))
        return (
            jnp.dot(tables[gh], hi, preferred_element_type=F32)
            + jnp.dot(tables[gh], lo, preferred_element_type=F32)
            + jnp.dot(tables[gl], hi, preferred_element_type=F32)
        ).T

    def chip_copy(i, h):
        k = 2 * i + h
        return remote(parts.at[k, 1 - core], d_recv.at[k], d_s, d_r.at[k], partner)

    def y_copy(i):
        return remote(y_send.at[i], y_recv.at[i], y_s, y_r.at[i], y_peer)

    def w_copy(i, j):
        dev = level(i) + j * (2 - 4 * x)
        place = x + j * (1 - 2 * x)
        slot = 3 + 2 * (last - differ(my_z, plane(i, my_z))) + j
        return remote(w_send.at[i, place], final.at[slot], w_s, final_r, dev)

    def v_copy():
        return remote(v_send, v_recv, v_s, v_r, level(far))

    def near_copy(j):
        src = sums.at[0, x] if j == 0 else sums.at[j - 1, 1 - x]
        return remote(src, final.at[j], n_s, final_r, near[j])

    def compute(i, h):
        with scope(f"halo{i}{h}"):
            @pl.when(has_prev & has_next)
            def _():
                both = halo_v.at[i, :, :, lanes(h)]
                remote(both, both, t_s, halo_r.at[2 * i + h], me).wait_recv()

            @pl.when(~has_next)
            def _():
                taps_copy(i, h, me).wait_recv()

            @pl.when(~has_prev)
            def _():
                hist_copy(i, h, me).wait_recv()

        at_step = steps.index((i, h))
        if at_step + AHEAD < len(steps):
            send_halo(at_step + AHEAD, up, down)

        with scope(f"comp{i}{h}"):
            at = lanes(h)
            both = halo_products(
                held(q0, i, at), held(q1, i, at), held(sh0, i, at), held(sh1, i, at), held(st1, i, at),
                forward(halo_v[i, 0, :, at]), forward(halo_v[i, 1, :, at]),
            )
            for side, spec in enumerate(both):
                res = inverse(spec)
                for k in range(res.shape[0] // block):
                    parts[2 * i + h, k % 2, k // 2, :, pl.ds(side * seg, seg)] = res[k * block : (k + 1) * block]
            chip_copy(i, h).start()

    def chip_sum(i, h):
        with scope(f"chip{i}{h if isinstance(h, int) else ''}"):
            chip_copy(i, h).wait_recv()
        return parts[2 * i + h, core] + d_recv[2 * i + h]

    def route_y(i):
        y_send[i] = chip_sum(i, 0)
        y_copy(i).start()

    def route_w(i):
        value = chip_sum(i, 1)
        if i < far:
            with scope(f"y{i}"):
                y_copy(i).wait_recv()
            value = value + y_recv[i]
        w_send[i] = value
        for j in (1, 0):
            w_copy(i, j).start()

    def route_v():
        v_send[...] = chip_sum(far, 0)
        v_copy().start()

    swap = me < PLANE // 2

    def spread():
        value = chip_sum(last, jnp.where(swap, 1, 0))
        with scope("v"):
            v_copy().wait_recv()
        sums[0] = value + v_recv[...]
        near_copy(0).start()
        near_copy(1).start()

    def finish():
        sums[1] = chip_sum(last, jnp.where(swap, 0, 1))
        near_copy(2).start()

    for i in range(nz):
        local(i)
        if i % 2:
            further(i // 2)
    compute(0, 0)
    compute(1, 0)
    for stage in range(nz // 2, nz - 1):
        further(stage)
    route_y(0)
    for i in range(2, last):
        compute(i, 0)
        route_y(i - 1)
    compute(0, 1)
    route_v()
    for i in range(1, last):
        compute(i, 1)
        if i < far:
            route_w(i - 1)
    compute(last, 0)
    route_w(far)
    compute(last, 1)
    pl.when(swap)(finish)
    route_w(far - 1)
    spread()
    pl.when(~swap)(finish)
    own = own_part()
    total = sums[1, x] + own
    with scope("final"):
        remote(final, final, n_s, final_r, me).wait_recv()
    for k in range(final.shape[0]):
        total = total + final[k]
    out[...] = rows_v[2] * total

    with scope("sends"):
        @pl.when(has_next)
        def _():
            remote(halo_v.at[:, 0], halo_v.at[:, 0], t_s, final_r, me).wait_send()

        @pl.when(has_prev)
        def _():
            remote(halo_v.at[:, 1], halo_v.at[:, 1], h_s, final_r, me).wait_send()

        three = final.at[pl.ds(0, 3)]
        for src, sem in ((d_recv, d_s), (y_send, y_s), (w_send, w_s), (v_send, v_s), (three, n_s)):
            remote(src, src, sem, final_r, me).wait_send()


def kernel_body(history, taps, self_taps, fresh, gate):
    n = lax.axis_size(AXIS)
    rows, channels = history.shape
    block, new_len = fresh.shape
    seg = new_len // 2
    nz = n // PLANE
    width = channels // nz
    fh, fl = halves(dft_matrix(seg))
    gh, gl = halves(dft_matrix(seg).T / seg)
    tables = np.concatenate([np.concatenate([fh, fh], axis=1), np.concatenate([fl, fl], axis=1), gh, gl], axis=0)
    vmem = pl.BlockSpec(memory_space=pltpu.VMEM)
    hbm = pl.BlockSpec(memory_space=pl.ANY)
    dma = pltpu.SemaphoreType.DMA
    spec = pltpu.VMEM((nz, 2 * seg, width), F32)
    far = nz - 2

    def pairs(*lead):
        return pltpu.VMEM((*lead, 2, block, new_len), F32)

    return pl.pallas_call(
        lambda *refs: kernel(n, seg, *refs),
        out_shape=pltpu.VMEM(fresh.shape, F32),
        in_specs=[hbm] * 6,
        out_specs=vmem,
        scratch_shapes=[
            pltpu.VMEM((3, block, new_len), F32),
            pltpu.VMEM(tables.shape, BF16),
            pltpu.VMEM((nz, 2, rows, width), F32),
            pltpu.VMEM((nz, 2, seg, width), F32),
            spec, spec, spec, spec, spec,
            pairs(2 * nz, 2), pairs(2 * nz),
            pairs(far), pairs(far), pairs(far + 1),
            pairs(), pairs(),
            pairs(2),
            pltpu.VMEM((3 + 2 * (far + 1), block, new_len), F32),
            pltpu.SemaphoreType.REGULAR((nz - 1,)),
            dma((2,)), dma((nz,)), dma,
            dma, dma, dma((2 * nz,)),
            dma, dma((2 * nz,)),
            dma, dma((far,)),
            dma,
            dma, dma,
            dma, dma,
        ],
        compiler_params=pltpu.CompilerParams(collective_id=0, has_side_effects=True),
        name="hyena",
    )(history, taps, self_taps, fresh, gate, jnp.asarray(tables))


def solution(mesh):
    n = mesh.shape[AXIS]

    def body(history, taps, self_taps, fresh, gate):
        channels = history.shape[1]
        block = fresh.shape[0]
        planes = n // PLANE
        fits = n % PLANE == 0 and planes >= 4 and planes & (planes - 1) == 0 and block % 32 == 0
        chosen = kernel_body if fits and channels == block * n else plain_body
        return chosen(history, taps, self_taps, fresh, gate)

    spec = P(AXIS, None)
    return jax.shard_map(body, mesh=mesh, in_specs=(spec,) * 5, out_specs=spec, check_vma=False)
```

```python
import math

import jax
import jax.numpy as jnp
import numpy as np
from jax import lax
from jax.experimental import pallas as pl
from jax.experimental.pallas import tpu as pltpu
from jax.sharding import PartitionSpec as P

AXIS = "seq"
PLANE = 8
MESH = pl.DeviceIdType.MESH
F32 = jnp.float32
BF16 = jnp.bfloat16
scope = jax.named_scope
AHEAD = 3


def dft_matrix(seg):
    phase = np.outer(4 * np.arange(seg) + 1, np.arange(seg)) % (4 * seg)
    angle = phase * (math.pi / (2 * seg))
    return np.concatenate([np.cos(angle), -np.sin(angle)], axis=0)


def halves(matrix):
    high = np.asarray(matrix, np.float32).astype(BF16)
    low = np.asarray(matrix - high.astype(np.float64), np.float32).astype(BF16)
    return high, low


def split(value):
    high = value.astype(BF16)
    return high, (value - high.astype(F32)).astype(BF16)


def mul_conj(a, b):
    return a[0] * b[0] + a[1] * b[1], a[1] * b[0] - a[0] * b[1]


def mul(a, b):
    return a[0] * b[0] - a[1] * b[1], a[0] * b[1] + a[1] * b[0]


def add(a, b):
    return a[0] + b[0], a[1] + b[1]


def turn(a):
    return -a[1], a[0]


def back(a):
    return a[1], -a[0]


def local_products(hs, ts):
    us = [None] + [add(ts[a], turn(ts[a - 1])) for a in range(1, len(ts))]
    first = mul_conj(hs[0], ts[0])
    for a in range(1, len(hs)):
        first = add(first, mul_conj(hs[a], us[a]))
    second = mul_conj(hs[1], ts[0])
    for a in range(2, len(hs)):
        second = add(second, mul_conj(hs[a], us[a - 1]))
    return first, second


def halo_products(first, second, h0, h1, t_near, t_before, h_after):
    one = mul_conj(h0, t_before)
    two = add(mul_conj(h1, t_before), mul_conj(h_after, t_near))
    return add(first, back(one)), add(add(second, one), back(two))


def own_products(f0, f1, s0, s1):
    first = mul(f0, s0)
    return first, add(turn(first), add(mul(f0, s1), mul(f1, s0)))


def plain_body(history, taps, self_taps, fresh, gate):
    n = lax.axis_size(AXIS)
    seg = fresh.shape[1] // 2
    matrix = jnp.asarray(dft_matrix(seg).astype(np.float32))
    hp = lax.Precision.HIGHEST
    before = lax.ppermute(taps[-seg:], AXIS, [(s, s + 1) for s in range(n - 1)])
    after = lax.ppermute(history[:seg], AXIS, [(s, s - 1) for s in range(1, n)])

    def forward(rows):
        spec = jnp.dot(matrix, rows, precision=hp)
        return spec[:seg], spec[seg:]

    def inverse(spec):
        return jnp.dot(matrix.T / seg, jnp.concatenate(spec, axis=0), precision=hp)

    count = history.shape[0] // seg
    hs = [forward(history[a * seg : (a + 1) * seg]) for a in range(count)]
    ts = [forward(taps[a * seg : (a + 1) * seg]) for a in range(count)]
    first, second = local_products(hs, ts)
    first, second = halo_products(first, second, hs[0], hs[1], ts[-2], forward(before), forward(after))
    part = jnp.concatenate([inverse(first), inverse(second)], axis=0).T
    summed = lax.psum_scatter(part, AXIS, scatter_dimension=0, tiled=True)
    f, s = fresh.T, self_taps.T
    own = own_products(forward(f[:seg]), forward(f[seg:]), forward(s[:seg]), forward(s[seg:]))
    own_part = jnp.concatenate([inverse(own[0]), inverse(own[1])], axis=0).T
    return gate * (summed + own_part)


def flip(z, mask):
    value, bit = z, 1
    while bit <= mask:
        if mask & bit:
            value = value + bit - 2 * bit * (z // bit % 2)
        bit *= 2
    return value


def kernel(n, seg, hist, taps, self_taps_h, fresh_h, gate_h, tables_h, out,
           rows_v, tables, both_v, halo_v, sh0, sh1, st1, q0, q1,
           parts, d_recv, y_send, y_recv, w_send, v_send, v_recv, sums, final,
           ready, small_sem, load_sem, edge_sem, t_s, h_s, halo_r, d_s, d_r, y_s, y_r, w_s, v_s, v_r, n_s, final_r):
    me = lax.axis_index(AXIS)
    nz = n // PLANE
    my_z, low = me // PLANE, me % PLANE
    core, x, y = me % 2, low // 2 % 2, low // 4
    rows = hist.shape[0]
    count = rows // seg
    width = hist.shape[1] // nz
    half = width // 2
    block = width // PLANE
    last = nz - 1
    far = nz - 2
    partner = me + 1 - 2 * core
    x_peer, y_peer = me + 2 - 4 * x, me + 4 - 8 * y
    diagonal = me + 2 - 4 * x + 4 - 8 * y
    near = (y_peer, diagonal, x_peer)
    steps = [(i, h) for h in range(2) for i in range(last)] + [(last, 0), (last, 1)]

    def plane(i, z):
        straight = flip(z, last - i)
        if i >= far:
            return straight
        low_first = flip(z, last - i // 2 * 2) // 2 * 2 + i % 2
        return jnp.where(z >= nz // 2, low_first, straight)

    def level(i):
        return me + (plane(i, my_z) - my_z) * PLANE

    def half_row(i, h, dev):
        row = (dev % PLANE // 4 + 1 + h) % 2
        return jnp.where(dev < PLANE, h, row) if i == last else row

    def cols(i, h, dev):
        base = plane(i, dev // PLANE) * width + half_row(i, h, dev) * half
        return pl.ds(pl.multiple_of(base, half), half)

    def differ(a, b):
        value, bit = 0, 1
        while bit < nz:
            value = value + bit * ((a // bit + b // bit) % 2)
            bit *= 2
        return value

    def lanes(h):
        return pl.ds(h * half, half)

    def remote(src, dst, send, recv, dev):
        return pltpu.make_async_remote_copy(
            src_ref=src, dst_ref=dst, send_sem=send, recv_sem=recv, device_id=(dev,), device_id_type=MESH
        )

    has_next, has_prev = me < n - 1, me > 0
    outer = me + 2 * core - 1
    has_outer = (outer >= 0) & (outer < n)
    up = has_next & (low == PLANE - 1)
    down = has_prev & (low == 0)
    beside = [partner, x_peer, x_peer + 1 - 2 * core, y_peer, y_peer + 1 - 2 * core]
    over = [me + PLANE, partner + PLANE]
    under = [me - PLANE, partner - PLANE]
    has_over, has_under = my_z < nz - 1, my_z > 0
    met = len(beside) + jnp.where(has_over, len(over), 0) + jnp.where(has_under, len(under), 0)

    def greet(sem):
        def tell(devices):
            for dev in devices:
                pl.semaphore_signal(sem, inc=1, device_id=(dev,), device_id_type=MESH)

        tell(beside)
        pl.when(has_over)(lambda: tell(over))
        pl.when(has_under)(lambda: tell(under))

    barrier = pltpu.get_barrier_semaphore()

    @pl.when(has_outer)
    def _():
        pl.semaphore_signal(barrier, inc=1, device_id=(outer,), device_id_type=MESH)

    greet(barrier)

    constants = pltpu.make_async_copy(tables_h, tables, small_sem.at[0])
    constants.start()

    def load(i, h, k, start, length, sem):
        span = pl.ds(start, length)
        pltpu.make_async_copy((hist, taps)[k].at[span, cols(i, h, me)], both_v.at[i, k, span, lanes(h)], sem).start()

    rest = rows - seg
    for i in range(nz):
        for h in range(2):
            load(i, h, 0, 0, seg, edge_sem)
            load(i, h, 1, rest, seg, edge_sem)
    for i in range(nz):
        for h in range(2):
            load(i, h, 0, seg, rest, load_sem.at[i])
            load(i, h, 1, 0, rest, load_sem.at[i])
    for k, src in enumerate((self_taps_h, fresh_h, gate_h)):
        pltpu.make_async_copy(src, rows_v.at[k], small_sem.at[1]).start()

    with scope("barrier"):
        pl.semaphore_wait(barrier, met + jnp.where(has_outer, 1, 0))
    greet(ready.at[0])
    pltpu.make_async_copy(halo_v, halo_v, edge_sem).wait()

    def mine(i, dev):
        goal = plane(i, dev // PLANE)
        mask = differ(my_z, goal)
        straight = last - mask
        return jnp.where((my_z >= nz // 2) & (mask >= 2), straight // 2 * 2 + goal % 2, straight)

    def spot(i, h, dev):
        row = half_row(i, h, dev)
        place = jnp.where((me < PLANE) & (plane(i, dev // PLANE) == my_z), row, (row + y + 1) % 2)
        return pl.ds(pl.multiple_of(place * half, half), half)

    def taps_copy(i, h, dev):
        src = both_v.at[mine(i, dev), 1, pl.ds(rows - seg, seg), spot(i, h, dev)]
        return remote(src, halo_v.at[i, 0, :, lanes(h)], t_s, halo_r.at[2 * i + h], dev)

    def hist_copy(i, h, dev):
        src = both_v.at[mine(i, dev), 0, pl.ds(0, seg), spot(i, h, dev)]
        return remote(src, halo_v.at[i, 1, :, lanes(h)], h_s, halo_r.at[2 * i + h], dev)

    def send_halo(k, forward_when, back_when):
        i, h = steps[k]

        @pl.when(forward_when)
        def _():
            taps_copy(i, h, me + 1).start()

        @pl.when(back_when)
        def _():
            hist_copy(i, h, me - 1).start()

    for k in range(len(steps)):
        if k < AHEAD:
            send_halo(k, has_next, has_prev)
        else:
            send_halo(k, has_next & ~up, has_prev & ~down)

    def further(stage):
        with scope(f"ready{stage}"):
            pl.semaphore_wait(ready.at[stage], met)
        if stage + 1 < nz - 1:
            greet(ready.at[stage + 1])

    fh, fl, gh, gl = (slice(k, k + r) for k, r in ((0, 2 * seg), (2 * seg, 2 * seg), (4 * seg, seg), (5 * seg, seg)))

    def forward(value):
        both = jnp.concatenate(split(value), axis=0)
        spec = jnp.dot(tables[fh], both, preferred_element_type=F32) + jnp.dot(
            tables[fl], both, preferred_element_type=F32
        )
        return spec[:seg], spec[seg:]

    def keep(ref, i, spec):
        ref[i, :seg], ref[i, seg:] = spec

    def held(ref, i, at):
        return ref[i, :seg, at], ref[i, seg:, at]

    @pl.when(me == 0)
    def _():
        halo_v[:, 0] = jnp.zeros_like(halo_v[:, 0])

    @pl.when(me == n - 1)
    def _():
        halo_v[:, 1] = jnp.zeros_like(halo_v[:, 1])

    constants.wait()

    def local(i):
        some = both_v.at[i, :, pl.ds(0, rest)]
        pltpu.make_async_copy(some, some, load_sem.at[i]).wait()
        with scope(f"local{i}"):
            hs = [forward(both_v[i, 0, pl.ds(a * seg, seg)]) for a in range(count)]
            ts = [forward(both_v[i, 1, pl.ds(a * seg, seg)]) for a in range(count)]
            first, second = local_products(hs, ts)
            keep(sh0, i, hs[0])
            keep(sh1, i, hs[1])
            keep(st1, i, ts[-2])
            keep(q0, i, first)
            keep(q1, i, second)

    contract = (((1,), (1,)), ((), ()))

    def dot_t(a, b):
        return lax.dot_general(a, b, contract, preferred_element_type=F32)

    def own_part():
        pltpu.make_async_copy(rows_v, rows_v, small_sem.at[1]).wait()
        s, f = rows_v[0], rows_v[1]
        both = jnp.concatenate(
            split(jnp.concatenate([f[:, :seg], f[:, seg:], s[:, :seg], s[:, seg:]], axis=0)), axis=1
        )
        spec = dot_t(both, tables[fh]) + dot_t(both, tables[fl])
        quads = [
            (spec[k * block : (k + 1) * block, :seg], spec[k * block : (k + 1) * block, seg:]) for k in range(4)
        ]
        a, b = own_products(*quads)
        high, low_half = split(
            jnp.concatenate([jnp.concatenate(a, axis=1), jnp.concatenate(b, axis=1)], axis=0)
        )
        res = dot_t(high, tables[gh]) + dot_t(low_half, tables[gh]) + dot_t(high, tables[gl])
        return jnp.concatenate([res[:block], res[block:]], axis=1)

    def inverse(spec):
        hi, lo = split(jnp.concatenate(spec, axis=0))
        return (
            jnp.dot(tables[gh], hi, preferred_element_type=F32)
            + jnp.dot(tables[gh], lo, preferred_element_type=F32)
            + jnp.dot(tables[gl], hi, preferred_element_type=F32)
        ).T

    def chip_copy(i, h):
        k = 2 * i + h
        return remote(parts.at[k, 1 - core], d_recv.at[k], d_s, d_r.at[k], partner)

    def y_copy(i):
        return remote(y_send.at[i], y_recv.at[i], y_s, y_r.at[i], y_peer)

    def w_copy(i, j):
        dev = level(i) + j * (2 - 4 * x)
        place = x + j * (1 - 2 * x)
        slot = 3 + 2 * (last - differ(my_z, plane(i, my_z))) + j
        return remote(w_send.at[i, place], final.at[slot], w_s, final_r, dev)

    def v_copy():
        return remote(v_send, v_recv, v_s, v_r, level(far))

    def near_copy(j):
        src = sums.at[0, x] if j == 0 else sums.at[j - 1, 1 - x]
        return remote(src, final.at[j], n_s, final_r, near[j])

    def compute(i, h):
        with scope(f"halo{i}{h}"):
            @pl.when(has_prev & has_next)
            def _():
                both = halo_v.at[i, :, :, lanes(h)]
                remote(both, both, t_s, halo_r.at[2 * i + h], me).wait_recv()

            @pl.when(~has_next)
            def _():
                taps_copy(i, h, me).wait_recv()

            @pl.when(~has_prev)
            def _():
                hist_copy(i, h, me).wait_recv()

        at_step = steps.index((i, h))
        if at_step + AHEAD < len(steps):
            send_halo(at_step + AHEAD, up, down)

        with scope(f"comp{i}{h}"):
            at = lanes(h)
            both = halo_products(
                held(q0, i, at), held(q1, i, at), held(sh0, i, at), held(sh1, i, at), held(st1, i, at),
                forward(halo_v[i, 0, :, at]), forward(halo_v[i, 1, :, at]),
            )
            for side, spec in enumerate(both):
                res = inverse(spec)
                for k in range(res.shape[0] // block):
                    parts[2 * i + h, k % 2, k // 2, :, pl.ds(side * seg, seg)] = res[k * block : (k + 1) * block]
            chip_copy(i, h).start()

    def chip_sum(i, h):
        with scope(f"chip{i}{h if isinstance(h, int) else ''}"):
            chip_copy(i, h).wait_recv()
        return parts[2 * i + h, core] + d_recv[2 * i + h]

    def route_y(i):
        y_send[i] = chip_sum(i, 0)
        y_copy(i).start()

    def route_w(i):
        value = chip_sum(i, 1)
        if i < far:
            with scope(f"y{i}"):
                y_copy(i).wait_recv()
            value = value + y_recv[i]
        w_send[i] = value
        for j in (1, 0):
            w_copy(i, j).start()

    def route_v():
        v_send[...] = chip_sum(far, 0)
        v_copy().start()

    swap = me < PLANE // 2

    def spread():
        value = chip_sum(last, jnp.where(swap, 1, 0))
        with scope("v"):
            v_copy().wait_recv()
        sums[0] = value + v_recv[...]
        near_copy(0).start()
        near_copy(1).start()

    def finish():
        sums[1] = chip_sum(last, jnp.where(swap, 0, 1))
        near_copy(2).start()

    for i in range(nz):
        local(i)
        if i % 2:
            further(i // 2)
    compute(0, 0)
    compute(1, 0)
    for stage in range(nz // 2, nz - 1):
        further(stage)
    route_y(0)
    for i in range(2, last):
        compute(i, 0)
        route_y(i - 1)
    compute(0, 1)
    route_v()
    for i in range(1, last):
        compute(i, 1)
        if i < far:
            route_w(i - 1)
    compute(last, 0)
    route_w(far)
    route_w(far - 1)
    compute(last, 1)
    pl.when(swap)(finish)
    spread()
    pl.when(~swap)(finish)
    own = own_part()
    total = sums[1, x] + own
    with scope("final"):
        remote(final, final, n_s, final_r, me).wait_recv()
    for k in range(final.shape[0]):
        total = total + final[k]
    out[...] = rows_v[2] * total

    with scope("sends"):
        @pl.when(has_next)
        def _():
            remote(halo_v.at[:, 0], halo_v.at[:, 0], t_s, final_r, me).wait_send()

        @pl.when(has_prev)
        def _():
            remote(halo_v.at[:, 1], halo_v.at[:, 1], h_s, final_r, me).wait_send()

        three = final.at[pl.ds(0, 3)]
        for src, sem in ((d_recv, d_s), (y_send, y_s), (w_send, w_s), (v_send, v_s), (three, n_s)):
            remote(src, src, sem, final_r, me).wait_send()


def kernel_body(history, taps, self_taps, fresh, gate):
    n = lax.axis_size(AXIS)
    rows, channels = history.shape
    block, new_len = fresh.shape
    seg = new_len // 2
    nz = n // PLANE
    width = channels // nz
    fh, fl = halves(dft_matrix(seg))
    gh, gl = halves(dft_matrix(seg).T / seg)
    tables = np.concatenate([np.concatenate([fh, fh], axis=1), np.concatenate([fl, fl], axis=1), gh, gl], axis=0)
    vmem = pl.BlockSpec(memory_space=pltpu.VMEM)
    hbm = pl.BlockSpec(memory_space=pl.ANY)
    dma = pltpu.SemaphoreType.DMA
    spec = pltpu.VMEM((nz, 2 * seg, width), F32)
    far = nz - 2

    def pairs(*lead):
        return pltpu.VMEM((*lead, 2, block, new_len), F32)

    return pl.pallas_call(
        lambda *refs: kernel(n, seg, *refs),
        out_shape=pltpu.VMEM(fresh.shape, F32),
        in_specs=[hbm] * 6,
        out_specs=vmem,
        scratch_shapes=[
            pltpu.VMEM((3, block, new_len), F32),
            pltpu.VMEM(tables.shape, BF16),
            pltpu.VMEM((nz, 2, rows, width), F32),
            pltpu.VMEM((nz, 2, seg, width), F32),
            spec, spec, spec, spec, spec,
            pairs(2 * nz, 2), pairs(2 * nz),
            pairs(far), pairs(far), pairs(far + 1),
            pairs(), pairs(),
            pairs(2),
            pltpu.VMEM((3 + 2 * (far + 1), block, new_len), F32),
            pltpu.SemaphoreType.REGULAR((nz - 1,)),
            dma((2,)), dma((nz,)), dma,
            dma, dma, dma((2 * nz,)),
            dma, dma((2 * nz,)),
            dma, dma((far,)),
            dma,
            dma, dma,
            dma, dma,
        ],
        compiler_params=pltpu.CompilerParams(collective_id=0, has_side_effects=True),
        name="hyena",
    )(history, taps, self_taps, fresh, gate, jnp.asarray(tables))


def solution(mesh):
    n = mesh.shape[AXIS]

    def body(history, taps, self_taps, fresh, gate):
        channels = history.shape[1]
        block = fresh.shape[0]
        planes = n // PLANE
        fits = n % PLANE == 0 and planes >= 4 and planes & (planes - 1) == 0 and block % 32 == 0
        chosen = kernel_body if fits and channels == block * n else plain_body
        return chosen(history, taps, self_taps, fresh, gate)

    spec = P(AXIS, None)
    return jax.shard_map(body, mesh=mesh, in_specs=(spec,) * 5, out_specs=spec, check_vma=False)
```
